32 devices in a mesh: rep: 4 (over y, x), fsdp: 8 (over z, core).
Axes of the slice: x: 2, y: 2, z: 4, core: 2. Of those that a mesh axis runs over, the one named last changes fastest.
Arguments:
- momentum: float32 [4, 18432, 2304], P('rep', 'fsdp'), may hold values from -60 to 60
- gradient: bfloat16 [4, 18432, 2304], P('rep', 'fsdp'), may hold values from -30 to 30
- right_factor: float32 [2304, 256], P('fsdp'), may hold values from -0.125 to 0.125
Outputs:
- new_momentum: float32 [4, 18432, 2304], P('rep', 'fsdp')
- update: bfloat16 [18432, 2304], P('fsdp')
- new_factor: float32 [2304, 256], P('fsdp')
The draws below stay inside these ranges and needn't reach their ends.
All inputs are finite; a program needn't handle non-finite values.
Results may differ from the reference program's by a relative error of at most 0.001.
Values sent between devices are 32-bit elements; how exact they have to be, the bound alone decides.
A program may use at most 128 MiB of HBM per device.

```python
import math
import jax
import jax.numpy as jnp
from jax import lax

ROWS = 18432
COLS = 2304
RANK = 256
REPLICAS = 4


def column_scales(key):
    scale_key = jax.random.fold_in(key, 11)
    rising = jnp.exp(jnp.log(10.0) * jnp.arange(COLS, dtype=jnp.float32) / COLS)
    jitter = jnp.exp(jax.random.uniform(scale_key, (COLS,), jnp.float32, -0.4, 0.4))
    return 0.3 * rising * jitter


def clipped_normal(key, shape):
    return jnp.clip(jax.random.normal(key, shape, jnp.float32), -6.0, 6.0)


def draw_momentum(key, part):
    scales = column_scales(key)
    values = 2.0 * clipped_normal(jax.random.fold_in(key, 1), (REPLICAS, ROWS, COLS)) * scales
    return values.astype(jnp.float32)


def draw_gradient(key, part):
    scales = column_scales(key)
    values = clipped_normal(jax.random.fold_in(key, 2), (REPLICAS, ROWS, COLS)) * scales
    return values.astype(jnp.bfloat16)


def level_of(stream_key, shape, shards, smallest, top_value):
    gain, own = 1.0, jax.random.fold_in(stream_key, 6)
    for dim, shards_of in shards:
        draws = jnp.exp(jax.random.uniform(jax.random.fold_in(own, dim), (shards_of,), jnp.float32, smallest / len(shards), top_value / len(shards)))
        gain = gain * jnp.repeat(draws, shape[dim] // shards_of).reshape([-1 if axis == dim else 1 for axis in range(len(shape))])
    return gain


def bell_draw(stream_key, dims, width, reach, cuts=(), held_as=jnp.bfloat16):
    entries = jax.random.normal(stream_key, dims, jnp.float32) * width
    if len(cuts) > 0:
        entries = level_of(stream_key, dims, cuts, -0.22, 0.18) * entries
    return jnp.clip(entries, min=-reach, max=reach).astype(held_as)


def setup_inputs(seed: int = 0) -> dict:
    key_of = jax.random.split(jax.random.key(seed), 4)
    momentum = draw_momentum(jax.random.fold_in(key_of[3], 71), 0)
    gradient = draw_gradient(jax.random.fold_in(key_of[3], 71), 0)
    right_factor = bell_draw(key_of[2], (COLS, RANK), COLS ** -0.5, 0.125, ((0, 8),), jnp.float32)
    return {"momentum": momentum, "gradient": gradient, "right_factor": right_factor}


epsilon = 1e-06
decay_rate = 0.95
highest = lax.Precision.HIGHEST

def reference(momentum, gradient, right_factor):
    buffer = momentum + gradient.astype(jnp.float32)
    projected = jnp.einsum('irc,ck->rk', buffer, right_factor, precision=highest)
    gram_matrix = jnp.dot(projected.T.astype(jnp.float32), projected.astype(jnp.float32), precision=highest, preferred_element_type=jnp.float32)
    lower_factor = jnp.linalg.cholesky(gram_matrix)
    orthonormal = jax.scipy.linalg.solve_triangular(lower_factor, projected.T, lower=True).T
    factor = jnp.einsum('irc,rk->ck', buffer, orthonormal, precision=highest) / REPLICAS
    col_norms = jnp.sqrt(lax.optimization_barrier(jnp.sum(factor * factor, axis=0)) + epsilon)
    new_factor = factor / col_norms
    correction = jnp.dot(orthonormal.astype(jnp.float32), factor.T.astype(jnp.float32), precision=highest, preferred_element_type=jnp.float32)
    new_momentum = buffer - (1.0 - decay_rate) * correction[None]
    scaled = math.sqrt(ROWS * COLS / RANK) * jnp.dot(orthonormal.astype(jnp.float32), new_factor.T.astype(jnp.float32), precision=highest, preferred_element_type=jnp.float32)
    return (new_momentum, scaled.astype(jnp.bfloat16), new_factor)
```

```python
import functools
import math

import jax
import jax.numpy as jnp
from jax import lax
from jax.experimental import pallas as pl
from jax.experimental.pallas import tpu as pltpu
from jax.sharding import PartitionSpec as P

epsilon = 1e-06
decay_rate = 0.95
highest = lax.Precision.HIGHEST
f32 = jnp.float32
bf16 = jnp.bfloat16
MESH = pl.DeviceIdType.MESH
VMEM_LIMIT = 60 * 1024 * 1024


def split(x):
    high = x.astype(bf16)
    return high, (x - high.astype(f32)).astype(bf16)


def dot(a, b, dims=(((1,), (0,)), ((), ()))):
    return lax.dot_general(a, b, dims, preferred_element_type=f32)


def exact(a, b, dims=(((1,), (0,)), ((), ()))):
    return lax.dot_general(a, b, dims, precision=highest, preferred_element_type=f32)


NT = (((1,), (1,)), ((), ()))
TN = (((0,), (0,)), ((), ()))


def greet(peers):
    barrier = pltpu.get_barrier_semaphore()
    for peer in peers:
        pl.semaphore_signal(barrier, inc=1, device_id=peer, device_id_type=MESH)
    pl.semaphore_wait(barrier, len(peers))


def remote(src, dst, send_sem, recv_sem, peer):
    copy = pltpu.make_async_remote_copy(
        src_ref=src, dst_ref=dst, send_sem=send_sem, recv_sem=recv_sem,
        device_id=peer, device_id_type=MESH,
    )
    copy.start()
    return copy


def gather_right(shard_n, own_ref, full_ref, send, recv, fsend, frecv, local):
    f = lax.axis_index("fsdp")
    r = lax.axis_index("rep")
    rows = own_ref.shape[0]
    chips = shard_n // 2
    chip, core = f // 2, lax.rem(f, 2)
    mate = (r, chip * 2 + 1 - core)
    others = [(r, lax.rem(chip + k, chips) * 2 + core) for k in range(1, chips)]
    greet([mate] + others)

    def block(index):
        return full_ref.at[pl.ds(pl.multiple_of(index * rows, 8), rows)]

    own = pltpu.make_async_copy(own_ref, block(f), local)
    own.start()
    copies = [remote(own_ref, block(f), send.at[k], recv.at[k], others[k]) for k in range(chips - 1)]
    passed = [remote(own_ref, block(f), fsend.at[0], frecv.at[0], mate)]
    for k in reversed(range(chips - 1)):
        copies[k].wait_recv()
        source = lax.rem(chip - (k + 1) + chips, chips) * 2 + core
        passed.append(remote(block(source), block(source), fsend.at[k + 1], frecv.at[k + 1], mate))
    for copy in copies:
        copy.wait_send()
    for copy in passed:
        copy.wait()
    own.wait()


def project(m_ref, g_ref, right_ref, out_ref, high, low):
    @pl.when(pl.program_id(0) == 0)
    def _():
        high[...], low[...] = split(right_ref[...])

    bh, bl = split(m_ref[0] + g_ref[0].astype(f32))
    out_ref[...] = dot(bh, high[...]) + dot(bh, low[...]) + dot(bl, high[...])


def inverse_small(a, size):
    row = lax.broadcasted_iota(jnp.int32, (size, 2 * size), 0)
    lane = lax.broadcasted_iota(jnp.int32, (size, 2 * size), 1)
    eye = jnp.where(row == lane - size, 1.0, 0.0).astype(f32)
    work = jnp.concatenate([a, eye[:, size:]], axis=1)
    for j in range(size):
        first = (j // 8) * 8
        pivot = work[j:j + 1, :]
        scaled = pivot / work[j:j + 1, j:j + 1]
        tail = work[first:, :]
        below = row[first:, :] > j
        tail = tail - jnp.where(below, tail[:, j:j + 1], 0.0) * scaled
        work = tail if first == 0 else jnp.concatenate([work[:first], tail], axis=0)
    diag = jnp.sum(jnp.where(row == lane, work, 0.0), axis=1, keepdims=True)
    return work[:, size:] * (1.0 / jnp.sqrt(diag))


def inverse_lower(a, size):
    if size <= 64:
        return inverse_small(a, size)
    h = size // 2
    top = inverse_lower(a[:h, :h], h)
    cross = exact(a[h:, :h], top, NT)
    low = inverse_lower(a[h:, h:] - exact(cross, cross, NT), h)
    corner = -exact(low, exact(cross, top))
    return jnp.concatenate(
        [jnp.concatenate([top, jnp.zeros((h, h), f32)], axis=1),
         jnp.concatenate([corner, low], axis=1)], axis=0)


def orthonormalize(reps, shard_n, part_ref, q_ref, full, xin, yin, xin2, yin2, gout, gin, gfull, inv,
                   send, recv, gsend, grecv, asend, arecv):
    r = lax.axis_index("rep")
    f = lax.axis_index("fsdp")
    rows, rank = part_ref.shape
    chunk = rows // reps
    half = rank // 2
    total = reps * shard_n
    me = r * shard_n + f
    sx = 1 - 2 * lax.rem(r, 2)
    sy = 1 - 2 * (r // 2)
    px, py, pd = r + sx, r + 2 * sy, r + sx + 2 * sy
    left, right = pl.ds(0, half), pl.ds(half, half)

    def of(index):
        return pl.ds(pl.multiple_of(index * chunk, 8), chunk)

    def device(k):
        d = lax.rem(me + k, total)
        return d, (d // shard_n, lax.rem(d, shard_n))

    peers = [device(k) for k in range(1, total)]
    greet([peer for _, peer in peers])

    s1 = [
        remote(part_ref.at[of(pd), left], xin.at[0], send.at[0], recv.at[0], (px, f)),
        remote(part_ref.at[of(pd), right], yin.at[0], send.at[1], recv.at[1], (py, f)),
        remote(part_ref.at[of(px), left], xin.at[1], send.at[2], recv.at[2], (px, f)),
        remote(part_ref.at[of(py), right], yin.at[1], send.at[3], recv.at[3], (py, f)),
    ]
    s1[0].wait_recv()
    xin[0] = xin[0] + part_ref[of(py), left]
    a = remote(xin.at[0], xin2, send.at[4], recv.at[4], (py, f))
    s1[1].wait_recv()
    yin[0] = yin[0] + part_ref[of(px), right]
    b = remote(yin.at[0], yin2, send.at[5], recv.at[5], (px, f))
    s1[2].wait_recv()
    xin[1] = xin[1] + part_ref[of(r), left]
    s1[3].wait_recv()
    yin[1] = yin[1] + part_ref[of(r), right]
    a.wait_recv()
    full[of(r), left] = xin[1] + xin2[...]
    b.wait_recv()
    full[of(r), right] = yin[1] + yin2[...]

    own = full[of(r), :]
    piece = rank // total
    gout[...] = exact(own, own, TN)

    def rows_of(index):
        return pl.ds(pl.multiple_of(index * piece, 8), piece)

    g1 = [
        remote(gout.at[rows_of(d)], gin.at[k], gsend.at[k], grecv.at[k], peer)
        for k, (d, peer) in enumerate(peers)
    ]
    acc = gout[rows_of(me), :]
    for k in range(total - 1):
        g1[k].wait_recv()
        acc = acc + gin[k]
    gfull[rows_of(me), :] = acc
    g2 = [
        remote(gfull.at[rows_of(me)], gfull.at[rows_of(me)], asend.at[k], arecv.at[k], peer)
        for k, (d, peer) in enumerate(peers)
    ]
    t1 = [
        remote(full.at[of(r), left], full.at[of(r), left], send.at[6], recv.at[6], (px, f)),
        remote(full.at[of(r), right], full.at[of(r), right], send.at[7], recv.at[7], (py, f)),
        remote(full.at[of(r), right], full.at[of(r), right], send.at[8], recv.at[8], (px, f)),
        remote(full.at[of(r), left], full.at[of(r), left], send.at[9], recv.at[9], (py, f)),
    ]
    for copy in g2:
        copy.wait_recv()
    t1[0].wait_recv()
    t2 = [remote(full.at[of(px), left], full.at[of(px), left], send.at[10], recv.at[10], (py, f))]
    t1[1].wait_recv()
    t2.append(remote(full.at[of(py), right], full.at[of(py), right], send.at[11], recv.at[11], (px, f)))
    inv[...] = inverse_lower(gfull[...], rank)
    t1[2].wait_recv()
    t1[3].wait_recv()
    t2[0].wait_recv()
    t2[1].wait_recv()
    for copy in s1 + [a, b] + g1 + g2 + t1 + t2:
        copy.wait_send()
    step = 256 if rows % 256 == 0 else chunk

    @pl.loop(0, rows // step)
    def _(i):
        at = pl.ds(pl.multiple_of(i * step, 8), step)
        q_ref[at, :] = exact(full[at, :], inv[...], NT)


def factor_term(m_ref, g_ref, q_ref, out_ref):
    bh, bl = split(m_ref[0] + g_ref[0].astype(f32))
    qh, ql = split(q_ref[...].T)
    term = dot(qh, bh) + dot(qh, bl) + dot(ql, bh)

    @pl.when(pl.program_id(0) == 0)
    def _():
        out_ref[...] = term

    @pl.when(pl.program_id(0) != 0)
    def _():
        out_ref[...] += term


def sum_factor(reps, shard_n, part_ref, out_ref, cin, xin, yin, xin2, yin2, zin, zsum, send, recv, zsend, zrecv):
    r = lax.axis_index("rep")
    f = lax.axis_index("fsdp")
    chips = shard_n // 2
    chip, core = f // 2, lax.rem(f, 2)
    rank, cols = part_ref.shape
    half = cols // 2
    left, right = pl.ds(0, half), pl.ds(half, half)
    sx = 1 - 2 * lax.rem(r, 2)
    sy = 1 - 2 * (r // 2)
    px, py, pd = r + sx, r + 2 * sy, r + sx + 2 * sy
    n0 = rank // 2
    n1 = n0 // reps
    n2 = n1 // chips
    mate = (r, chip * 2 + 1 - core)
    zs = [lax.rem(chip + k, chips) for k in range(1, chips)]
    greet([mate, (px, f), (py, f)] + [(r, z * 2 + core) for z in zs])

    def of(index):
        return pl.ds(pl.multiple_of(index * n1, 8), n1)

    mine = core * n0
    order = [pd, px, py, r]
    c = []
    for k, which in enumerate(order):
        away = pl.ds(pl.multiple_of((1 - core) * n0 + which * n1, 8), n1)
        c.append(remote(part_ref.at[away], cin.at[of(which)], send.at[k], recv.at[k], mate))

    def add_own(which):
        at = pl.ds(pl.multiple_of(mine + which * n1, 8), n1)
        cin[of(which), :] = cin[of(which), :] + part_ref[at, :]

    c[0].wait_recv()
    add_own(pd)
    s1 = [
        remote(cin.at[of(pd), left], xin.at[0], send.at[4], recv.at[4], (px, f)),
        remote(cin.at[of(pd), right], yin.at[0], send.at[5], recv.at[5], (py, f)),
    ]
    c[1].wait_recv()
    add_own(px)
    s1.append(remote(cin.at[of(px), left], xin.at[1], send.at[6], recv.at[6], (px, f)))
    c[2].wait_recv()
    add_own(py)
    s1.append(remote(cin.at[of(py), right], yin.at[1], send.at[7], recv.at[7], (py, f)))
    c[3].wait_recv()
    add_own(r)
    s1[0].wait_recv()
    xin[0] = xin[0] + cin[of(py), left]
    a = remote(xin.at[0], xin2, send.at[8], recv.at[8], (py, f))
    s1[1].wait_recv()
    yin[0] = yin[0] + cin[of(px), right]
    b = remote(yin.at[0], yin2, send.at[9], recv.at[9], (px, f))
    s1[2].wait_recv()
    xin[1] = xin[1] + cin[of(r), left]
    s1[3].wait_recv()
    yin[1] = yin[1] + cin[of(r), right]
    a.wait_recv()
    zsum[:, left] = xin[1] + xin2[...]
    b.wait_recv()
    zsum[:, right] = yin[1] + yin2[...]
    z1 = []
    for k, z in enumerate(zs):
        rows = pl.ds(pl.multiple_of(z * n2, 8), n2)
        z1.append(remote(zsum.at[rows], zin.at[k], zsend.at[k], zrecv.at[k], (r, z * 2 + core)))
    acc = zsum[pl.ds(pl.multiple_of(chip * n2, 8), n2), :]
    for k in range(chips - 1):
        z1[k].wait_recv()
        acc = acc + zin[k]

    def block(rep, z, co):
        return pl.ds(pl.multiple_of(co * n0 + rep * n1 + z * n2, 8), n2)

    def group(rep, co):
        return pl.ds(pl.multiple_of(co * n0 + rep * n1, 8), n1)

    at = block(r, chip, core)
    out_ref[at, :] = acc * (1.0 / reps)
    z2 = [
        remote(out_ref.at[at], out_ref.at[at], zsend.at[chips + k], zrecv.at[chips + k], (r, z * 2 + core))
        for k, z in enumerate(zs)
    ]
    for copy in z2:
        copy.wait_recv()
    whole = group(r, core)
    t = [
        remote(out_ref.at[whole, left], out_ref.at[whole, left], send.at[10], recv.at[10], (px, f)),
        remote(out_ref.at[whole, right], out_ref.at[whole, right], send.at[11], recv.at[11], (py, f)),
        remote(out_ref.at[whole, right], out_ref.at[whole, right], send.at[12], recv.at[12], (px, f)),
        remote(out_ref.at[whole, left], out_ref.at[whole, left], send.at[13], recv.at[13], (py, f)),
        remote(out_ref.at[whole], out_ref.at[whole], send.at[14], recv.at[14], mate),
    ]
    t[0].wait_recv()
    gx, gy, gd = group(px, core), group(py, core), group(pd, core)
    t.append(remote(out_ref.at[gx, left], out_ref.at[gx, left], send.at[15], recv.at[15], (py, f)))
    t[1].wait_recv()
    t.append(remote(out_ref.at[gy, right], out_ref.at[gy, right], send.at[16], recv.at[16], (px, f)))
    t[2].wait_recv()
    t.append(remote(out_ref.at[gx], out_ref.at[gx], send.at[17], recv.at[17], mate))
    t[3].wait_recv()
    t.append(remote(out_ref.at[gy], out_ref.at[gy], send.at[18], recv.at[18], mate))
    t[5].wait_recv()
    t[6].wait_recv()
    t.append(remote(out_ref.at[gd], out_ref.at[gd], send.at[19], recv.at[19], mate))
    for index in (4, 7, 8, 9):
        t[index].wait_recv()
    for copy in c + s1 + [a, b] + z1 + z2 + t:
        copy.wait_send()


def finish(scale, m_ref, g_ref, q_ref, factor_ref, mom_ref, upd_ref, new_ref, plain, high, low):
    @pl.when(pl.program_id(0) == 0)
    def _():
        factor = factor_ref[...]
        norms = jnp.sqrt(jnp.sum(factor * factor, axis=1, keepdims=True) + epsilon)
        new = factor / norms
        new_ref[...] = new
        plain[...] = ((1.0 - decay_rate) * factor).astype(bf16)
        high[...], low[...] = split(new)

    qh, ql = split(q_ref[...])
    mom_ref[0] = (m_ref[0] + g_ref[0].astype(f32)) - dot(qh, plain[...])
    direction = dot(qh, high[...]) + dot(qh, low[...]) + dot(ql, high[...])
    upd_ref[...] = (scale * direction).astype(bf16)


def params(**more):
    return pltpu.CompilerParams(vmem_limit_bytes=VMEM_LIMIT, **more)


def by_kernels(reps, shard_n, total_rows, momentum, gradient, right_factor):
    _, rows, cols = momentum.shape
    rank = right_factor.shape[1]
    tile = 256 if rows % 256 == 0 else rows // 8
    steps = rows // tile
    vmem = pl.BlockSpec(memory_space=pltpu.VMEM)
    dma = pltpu.SemaphoreType.DMA
    chips = shard_n // 2

    def stripe(width):
        return pl.BlockSpec((tile, width), lambda i: (i, 0))

    cube = pl.BlockSpec((1, tile, cols), lambda i: (0, i, 0))

    def fixed(*shape):
        return pl.BlockSpec(shape, lambda i: (0,) * len(shape))

    right = pl.pallas_call(
        functools.partial(gather_right, shard_n),
        out_shape=jax.ShapeDtypeStruct((cols, rank), f32),
        in_specs=[vmem], out_specs=vmem,
        scratch_shapes=[dma((chips,)), dma((chips,)), dma((chips,)), dma((chips,)), dma],
        compiler_params=params(collective_id=0, has_side_effects=True),
        name="gather_right",
    )(right_factor)
    partial = pl.pallas_call(
        project,
        grid=(steps,),
        out_shape=jax.ShapeDtypeStruct((rows, rank), f32),
        in_specs=[cube, cube, fixed(cols, rank)], out_specs=stripe(rank),
        scratch_shapes=[pltpu.VMEM((cols, rank), bf16)] * 2,
        compiler_params=params(), name="project",
    )(momentum, gradient, right)
    chunk, total = rows // reps, reps * shard_n
    orthonormal = pl.pallas_call(
        functools.partial(orthonormalize, reps, shard_n),
        out_shape=jax.ShapeDtypeStruct((rows, rank), f32),
        in_specs=[vmem], out_specs=vmem,
        scratch_shapes=[
            pltpu.VMEM((rows, rank), f32),
            pltpu.VMEM((2, chunk, rank // 2), f32), pltpu.VMEM((2, chunk, rank // 2), f32),
            pltpu.VMEM((chunk, rank // 2), f32), pltpu.VMEM((chunk, rank // 2), f32),
            pltpu.VMEM((rank, rank), f32),
            pltpu.VMEM((total, rank // total, rank), f32),
            pltpu.VMEM((rank, rank), f32), pltpu.VMEM((rank, rank), f32),
            dma((12,)), dma((12,)), dma((total,)), dma((total,)), dma((total,)), dma((total,)),
        ],
        compiler_params=params(collective_id=1, has_side_effects=True),
        name="orthonormalize",
    )(partial)
    term = pl.pallas_call(
        factor_term,
        grid=(steps,),
        out_shape=jax.ShapeDtypeStruct((rank, cols), f32),
        in_specs=[cube, cube, stripe(rank)], out_specs=fixed(rank, cols),
        compiler_params=params(), name="factor_term",
    )(momentum, gradient, orthonormal)
    n1 = rank // 2 // reps
    factor = pl.pallas_call(
        functools.partial(sum_factor, reps, shard_n),
        out_shape=jax.ShapeDtypeStruct((rank, cols), f32),
        in_specs=[vmem], out_specs=vmem,
        scratch_shapes=[
            pltpu.VMEM((rank // 2, cols), f32),
            pltpu.VMEM((2, n1, cols // 2), f32), pltpu.VMEM((2, n1, cols // 2), f32),
            pltpu.VMEM((n1, cols // 2), f32), pltpu.VMEM((n1, cols // 2), f32),
            pltpu.VMEM((chips, n1 // chips, cols), f32), pltpu.VMEM((n1, cols), f32),
            dma((20,)), dma((20,)), dma((2 * chips,)), dma((2 * chips,)),
        ],
        compiler_params=params(collective_id=2, has_side_effects=True),
        name="sum_factor",
    )(term)
    new_momentum, update, new = pl.pallas_call(
        functools.partial(finish, math.sqrt(total_rows * cols / rank)),
        grid=(steps,),
        out_shape=(
            jax.ShapeDtypeStruct(momentum.shape, f32),
            jax.ShapeDtypeStruct((rows, cols), bf16),
            jax.ShapeDtypeStruct((rank, cols), f32),
        ),
        in_specs=[cube, cube, stripe(rank), fixed(rank, cols)],
        out_specs=(cube, stripe(cols), fixed(rank, cols)),
        scratch_shapes=[pltpu.VMEM((rank, cols), bf16)] * 3,
        compiler_params=params(), name="finish",
    )(momentum, gradient, orthonormal, factor)
    own = cols // shard_n
    new_factor = lax.dynamic_slice_in_dim(new, lax.axis_index("fsdp") * own, own, axis=1).T
    return new_momentum, update, new_factor


def by_collectives(reps, shard_n, total_rows, momentum, gradient, right_factor):
    buffer = momentum[0] + gradient[0].astype(f32)
    partial = exact(buffer, lax.all_gather(right_factor, "fsdp", axis=0, tiled=True))
    projected = lax.psum(partial, "rep")
    gram_matrix = lax.psum(exact(projected, projected, TN), "fsdp")
    lower_factor = jnp.linalg.cholesky(gram_matrix)
    orthonormal = jax.scipy.linalg.solve_triangular(lower_factor, projected.T, lower=True).T
    scattered = lax.psum_scatter(
        exact(buffer, orthonormal, TN), "fsdp", scatter_dimension=0, tiled=True)
    own_factor = lax.psum(scattered, "rep") / reps
    full_factor = lax.all_gather(own_factor, "fsdp", axis=0, tiled=True)
    col_norms = jnp.sqrt(jnp.sum(full_factor * full_factor, axis=0) + epsilon)
    new_factor = own_factor / col_norms
    correction = exact(orthonormal, full_factor, NT)
    new_momentum = (buffer - (1.0 - decay_rate) * correction)[None]
    direction = exact(orthonormal, full_factor / col_norms, NT)
    scale = math.sqrt(total_rows * buffer.shape[1] / right_factor.shape[1])
    return new_momentum, (scale * direction).astype(bf16), new_factor


def solution(mesh):
    reps, shard_n = mesh.shape["rep"], mesh.shape["fsdp"]

    def shards(momentum, gradient, right_factor):
        rows, cols = momentum.shape[1:]
        rank = right_factor.shape[1]
        fits = (
            reps == 4 and shard_n % 2 == 0 and shard_n > 2 and rows % 128 == 0
            and (cols // shard_n) % 8 == 0 and cols % 256 == 0
            and rank % (8 * reps * shard_n) == 0
        )
        run = by_kernels if fits else by_collectives
        return run(reps, shard_n, rows * shard_n, momentum, gradient, right_factor)

    in_specs = (P("rep", "fsdp", None), P("rep", "fsdp", None), P("fsdp", None))
    out_specs = (P("rep", "fsdp", None), P("fsdp", None), P("fsdp", None))
    return jax.shard_map(shards, mesh=mesh, in_specs=in_specs, out_specs=out_specs, check_vma=False)
```

```python
import functools
import math

import jax
import jax.numpy as jnp
from jax import lax
from jax.experimental import pallas as pl
from jax.experimental.pallas import tpu as pltpu
from jax.sharding import PartitionSpec as P

epsilon = 1e-06
decay_rate = 0.95
highest = lax.Precision.HIGHEST
f32 = jnp.float32
bf16 = jnp.bfloat16
MESH = pl.DeviceIdType.MESH
VMEM_LIMIT = 60 * 1024 * 1024


def split(x):
    high = x.astype(bf16)
    return high, (x - high.astype(f32)).astype(bf16)


def dot(a, b, dims=(((1,), (0,)), ((), ()))):
    return lax.dot_general(a, b, dims, preferred_element_type=f32)


def exact(a, b, dims=(((1,), (0,)), ((), ()))):
    return lax.dot_general(a, b, dims, precision=highest, preferred_element_type=f32)


NT = (((1,), (1,)), ((), ()))
TN = (((0,), (0,)), ((), ()))


def greet(peers):
    barrier = pltpu.get_barrier_semaphore()
    for peer in peers:
        pl.semaphore_signal(barrier, inc=1, device_id=peer, device_id_type=MESH)
    pl.semaphore_wait(barrier, len(peers))


def remote(src, dst, send_sem, recv_sem, peer):
    copy = pltpu.make_async_remote_copy(
        src_ref=src, dst_ref=dst, send_sem=send_sem, recv_sem=recv_sem,
        device_id=peer, device_id_type=MESH,
    )
    copy.start()
    return copy


def gather_right(shard_n, own_ref, full_ref, send, recv, fsend, frecv, local):
    f = lax.axis_index("fsdp")
    r = lax.axis_index("rep")
    rows = own_ref.shape[0]
    chips = shard_n // 2
    chip, core = f // 2, lax.rem(f, 2)
    mate = (r, chip * 2 + 1 - core)
    others = [(r, lax.rem(chip + k, chips) * 2 + core) for k in range(1, chips)]
    greet([mate] + others)

    def block(index):
        return full_ref.at[pl.ds(pl.multiple_of(index * rows, 8), rows)]

    own = pltpu.make_async_copy(own_ref, block(f), local)
    own.start()
    copies = [remote(own_ref, block(f), send.at[k], recv.at[k], others[k]) for k in range(chips - 1)]
    passed = [remote(own_ref, block(f), fsend.at[0], frecv.at[0], mate)]
    for k in reversed(range(chips - 1)):
        copies[k].wait_recv()
        source = lax.rem(chip - (k + 1) + chips, chips) * 2 + core
        passed.append(remote(block(source), block(source), fsend.at[k + 1], frecv.at[k + 1], mate))
    for copy in copies:
        copy.wait_send()
    for copy in passed:
        copy.wait()
    own.wait()


def project(m_ref, g_ref, right_ref, out_ref, high, low):
    @pl.when(pl.program_id(0) == 0)
    def _():
        high[...], low[...] = split(right_ref[...])

    bh, bl = split(m_ref[0] + g_ref[0].astype(f32))
    out_ref[...] = dot(bh, high[...]) + dot(bh, low[...]) + dot(bl, high[...])


def inverse_small(a, size):
    row = lax.broadcasted_iota(jnp.int32, (size, 2 * size), 0)
    lane = lax.broadcasted_iota(jnp.int32, (size, 2 * size), 1)
    eye = jnp.where(row == lane - size, 1.0, 0.0).astype(f32)
    work = jnp.concatenate([a, eye[:, size:]], axis=1)
    for j in range(size):
        first = (j // 8) * 8
        pivot = work[j:j + 1, :]
        scaled = pivot / work[j:j + 1, j:j + 1]
        tail = work[first:, :]
        below = row[first:, :] > j
        tail = tail - jnp.where(below, tail[:, j:j + 1], 0.0) * scaled
        work = tail if first == 0 else jnp.concatenate([work[:first], tail], axis=0)
    diag = jnp.sum(jnp.where(row == lane, work, 0.0), axis=1, keepdims=True)
    return work[:, size:] * (1.0 / jnp.sqrt(diag))


def inverse_lower(a, size):
    if size <= 64:
        return inverse_small(a, size)
    h = size // 2
    top = inverse_lower(a[:h, :h], h)
    cross = exact(a[h:, :h], top, NT)
    low = inverse_lower(a[h:, h:] - exact(cross, cross, NT), h)
    corner = -exact(low, exact(cross, top))
    return jnp.concatenate(
        [jnp.concatenate([top, jnp.zeros((h, h), f32)], axis=1),
         jnp.concatenate([corner, low], axis=1)], axis=0)


def orthonormalize(reps, shard_n, part_ref, q_ref, full, xin, yin, xin2, yin2, gout, gin, gfull, inv,
                   send, recv, gsend, grecv, asend, arecv):
    r = lax.axis_index("rep")
    f = lax.axis_index("fsdp")
    rows, rank = part_ref.shape
    chunk = rows // reps
    half = rank // 2
    total = reps * shard_n
    me = r * shard_n + f
    sx = 1 - 2 * lax.rem(r, 2)
    sy = 1 - 2 * (r // 2)
    px, py, pd = r + sx, r + 2 * sy, r + sx + 2 * sy
    left, right = pl.ds(0, half), pl.ds(half, half)

    def of(index):
        return pl.ds(pl.multiple_of(index * chunk, 8), chunk)

    def device(k):
        d = lax.rem(me + k, total)
        return d, (d // shard_n, lax.rem(d, shard_n))

    peers = [device(k) for k in range(1, total)]
    greet([peer for _, peer in peers])

    s1 = [
        remote(part_ref.at[of(pd), left], xin.at[0], send.at[0], recv.at[0], (px, f)),
        remote(part_ref.at[of(pd), right], yin.at[0], send.at[1], recv.at[1], (py, f)),
        remote(part_ref.at[of(px), left], xin.at[1], send.at[2], recv.at[2], (px, f)),
        remote(part_ref.at[of(py), right], yin.at[1], send.at[3], recv.at[3], (py, f)),
    ]
    s1[0].wait_recv()
    xin[0] = xin[0] + part_ref[of(py), left]
    a = remote(xin.at[0], xin2, send.at[4], recv.at[4], (py, f))
    s1[1].wait_recv()
    yin[0] = yin[0] + part_ref[of(px), right]
    b = remote(yin.at[0], yin2, send.at[5], recv.at[5], (px, f))
    s1[2].wait_recv()
    xin[1] = xin[1] + part_ref[of(r), left]
    s1[3].wait_recv()
    yin[1] = yin[1] + part_ref[of(r), right]
    a.wait_recv()
    full[of(r), left] = xin[1] + xin2[...]
    b.wait_recv()
    full[of(r), right] = yin[1] + yin2[...]

    own = full[of(r), :]
    piece = rank // total
    gout[...] = exact(own, own, TN)

    def rows_of(index):
        return pl.ds(pl.multiple_of(index * piece, 8), piece)

    g1 = [
        remote(gout.at[rows_of(d)], gin.at[k], gsend.at[k], grecv.at[k], peer)
        for k, (d, peer) in enumerate(peers)
    ]
    acc = gout[rows_of(me), :]
    for k in range(total - 1):
        g1[k].wait_recv()
        acc = acc + gin[k]
    gfull[rows_of(me), :] = acc
    g2 = [
        remote(gfull.at[rows_of(me)], gfull.at[rows_of(me)], asend.at[k], arecv.at[k], peer)
        for k, (d, peer) in enumerate(peers)
    ]
    t1 = [
        remote(full.at[of(r), left], full.at[of(r), left], send.at[6], recv.at[6], (px, f)),
        remote(full.at[of(r), right], full.at[of(r), right], send.at[7], recv.at[7], (py, f)),
        remote(full.at[of(r), right], full.at[of(r), right], send.at[8], recv.at[8], (px, f)),
        remote(full.at[of(r), left], full.at[of(r), left], send.at[9], recv.at[9], (py, f)),
    ]
    for copy in g2:
        copy.wait_recv()
    t1[0].wait_recv()
    t2 = [remote(full.at[of(px), left], full.at[of(px), left], send.at[10], recv.at[10], (py, f))]
    t1[1].wait_recv()
    t2.append(remote(full.at[of(py), right], full.at[of(py), right], send.at[11], recv.at[11], (px, f)))
    inv[...] = inverse_lower(gfull[...], rank)
    t1[2].wait_recv()
    t1[3].wait_recv()
    t2[0].wait_recv()
    t2[1].wait_recv()
    for copy in s1 + [a, b] + g1 + g2 + t1 + t2:
        copy.wait_send()
    step = 256 if rows % 256 == 0 else chunk

    @pl.loop(0, rows // step)
    def _(i):
        at = pl.ds(pl.multiple_of(i * step, 8), step)
        q_ref[at, :] = exact(full[at, :], inv[...], NT)


def factor_term(m_ref, g_ref, q_ref, out_ref):
    bh, bl = split(m_ref[0] + g_ref[0].astype(f32))
    qh, ql = split(q_ref[...].T)
    term = dot(jnp.concatenate([qh, qh, ql], axis=1), jnp.concatenate([bh, bl, bh], axis=0))

    @pl.when(pl.program_id(0) == 0)
    def _():
        out_ref[...] = term

    @pl.when(pl.program_id(0) != 0)
    def _():
        out_ref[...] += term


def sum_factor(reps, shard_n, part_ref, out_ref, cin, xin, yin, xin2, yin2, zin, zsum, send, recv, zsend, zrecv):
    r = lax.axis_index("rep")
    f = lax.axis_index("fsdp")
    chips = shard_n // 2
    chip, core = f // 2, lax.rem(f, 2)
    rank, cols = part_ref.shape
    half = cols // 2
    left, right = pl.ds(0, half), pl.ds(half, half)
    sx = 1 - 2 * lax.rem(r, 2)
    sy = 1 - 2 * (r // 2)
    px, py, pd = r + sx, r + 2 * sy, r + sx + 2 * sy
    n0 = rank // 2
    n1 = n0 // reps
    n2 = n1 // chips
    mate = (r, chip * 2 + 1 - core)
    zs = [lax.rem(chip + k, chips) for k in range(1, chips)]
    greet([mate, (px, f), (py, f)] + [(r, z * 2 + core) for z in zs])

    def of(index):
        return pl.ds(pl.multiple_of(index * n1, 8), n1)

    mine = core * n0
    order = [pd, px, py, r]
    c = []
    for k, which in enumerate(order):
        away = pl.ds(pl.multiple_of((1 - core) * n0 + which * n1, 8), n1)
        c.append(remote(part_ref.at[away], cin.at[of(which)], send.at[k], recv.at[k], mate))

    def add_own(which):
        at = pl.ds(pl.multiple_of(mine + which * n1, 8), n1)
        cin[of(which), :] = cin[of(which), :] + part_ref[at, :]

    c[0].wait_recv()
    add_own(pd)
    s1 = [
        remote(cin.at[of(pd), left], xin.at[0], send.at[4], recv.at[4], (px, f)),
        remote(cin.at[of(pd), right], yin.at[0], send.at[5], recv.at[5], (py, f)),
    ]
    c[1].wait_recv()
    add_own(px)
    s1.append(remote(cin.at[of(px), left], xin.at[1], send.at[6], recv.at[6], (px, f)))
    c[2].wait_recv()
    add_own(py)
    s1.append(remote(cin.at[of(py), right], yin.at[1], send.at[7], recv.at[7], (py, f)))
    c[3].wait_recv()
    add_own(r)
    s1[0].wait_recv()
    xin[0] = xin[0] + cin[of(py), left]
    a = remote(xin.at[0], xin2, send.at[8], recv.at[8], (py, f))
    s1[1].wait_recv()
    yin[0] = yin[0] + cin[of(px), right]
    b = remote(yin.at[0], yin2, send.at[9], recv.at[9], (px, f))
    s1[2].wait_recv()
    xin[1] = xin[1] + cin[of(r), left]
    s1[3].wait_recv()
    yin[1] = yin[1] + cin[of(r), right]
    a.wait_recv()
    zsum[:, left] = xin[1] + xin2[...]
    b.wait_recv()
    zsum[:, right] = yin[1] + yin2[...]
    z1 = []
    for k, z in enumerate(zs):
        rows = pl.ds(pl.multiple_of(z * n2, 8), n2)
        z1.append(remote(zsum.at[rows], zin.at[k], zsend.at[k], zrecv.at[k], (r, z * 2 + core)))
    acc = zsum[pl.ds(pl.multiple_of(chip * n2, 8), n2), :]
    for k in range(chips - 1):
        z1[k].wait_recv()
        acc = acc + zin[k]

    def block(rep, z, co):
        return pl.ds(pl.multiple_of(co * n0 + rep * n1 + z * n2, 8), n2)

    def group(rep, co):
        return pl.ds(pl.multiple_of(co * n0 + rep * n1, 8), n1)

    at = block(r, chip, core)
    out_ref[at, :] = acc * (1.0 / reps)
    z2 = [
        remote(out_ref.at[at], out_ref.at[at], zsend.at[chips + k], zrecv.at[chips + k], (r, z * 2 + core))
        for k, z in enumerate(zs)
    ]
    for copy in z2:
        copy.wait_recv()
    whole = group(r, core)
    t = [
        remote(out_ref.at[whole, left], out_ref.at[whole, left], send.at[10], recv.at[10], (px, f)),
        remote(out_ref.at[whole, right], out_ref.at[whole, right], send.at[11], recv.at[11], (py, f)),
        remote(out_ref.at[whole, right], out_ref.at[whole, right], send.at[12], recv.at[12], (px, f)),
        remote(out_ref.at[whole, left], out_ref.at[whole, left], send.at[13], recv.at[13], (py, f)),
        remote(out_ref.at[whole], out_ref.at[whole], send.at[14], recv.at[14], mate),
    ]
    t[0].wait_recv()
    gx, gy, gd = group(px, core), group(py, core), group(pd, core)
    t.append(remote(out_ref.at[gx, left], out_ref.at[gx, left], send.at[15], recv.at[15], (py, f)))
    t[1].wait_recv()
    t.append(remote(out_ref.at[gy, right], out_ref.at[gy, right], send.at[16], recv.at[16], (px, f)))
    t[2].wait_recv()
    t.append(remote(out_ref.at[gx], out_ref.at[gx], send.at[17], recv.at[17], mate))
    t[3].wait_recv()
    t.append(remote(out_ref.at[gy], out_ref.at[gy], send.at[18], recv.at[18], mate))
    t[5].wait_recv()
    t[6].wait_recv()
    t.append(remote(out_ref.at[gd], out_ref.at[gd], send.at[19], recv.at[19], mate))
    for index in (4, 7, 8, 9):
        t[index].wait_recv()
    for copy in c + s1 + [a, b] + z1 + z2 + t:
        copy.wait_send()


def finish(scale, m_ref, g_ref, q_ref, factor_ref, mom_ref, upd_ref, new_ref, plain, pieces):
    @pl.when(pl.program_id(0) == 0)
    def _():
        factor = factor_ref[...]
        norms = jnp.sqrt(jnp.sum(factor * factor, axis=1, keepdims=True) + epsilon)
        new = factor / norms
        new_ref[...] = new
        plain[...] = ((1.0 - decay_rate) * factor).astype(bf16)
        high, low = split(new)
        pieces[...] = jnp.concatenate([high, low, high], axis=0)

    qh, ql = split(q_ref[...])
    mom_ref[0] = (m_ref[0] + g_ref[0].astype(f32)) - dot(qh, plain[...])
    direction = dot(jnp.concatenate([qh, qh, ql], axis=1), pieces[...])
    upd_ref[...] = (scale * direction).astype(bf16)


def params(**more):
    return pltpu.CompilerParams(vmem_limit_bytes=VMEM_LIMIT, **more)


def by_kernels(reps, shard_n, total_rows, momentum, gradient, right_factor):
    _, rows, cols = momentum.shape
    rank = right_factor.shape[1]
    tile = 256 if rows % 256 == 0 else rows // 8
    steps = rows // tile
    vmem = pl.BlockSpec(memory_space=pltpu.VMEM)
    dma = pltpu.SemaphoreType.DMA
    chips = shard_n // 2

    def stripe(width):
        return pl.BlockSpec((tile, width), lambda i: (i, 0))

    cube = pl.BlockSpec((1, tile, cols), lambda i: (0, i, 0))

    def fixed(*shape):
        return pl.BlockSpec(shape, lambda i: (0,) * len(shape))

    right = pl.pallas_call(
        functools.partial(gather_right, shard_n),
        out_shape=jax.ShapeDtypeStruct((cols, rank), f32),
        in_specs=[vmem], out_specs=vmem,
        scratch_shapes=[dma((chips,)), dma((chips,)), dma((chips,)), dma((chips,)), dma],
        compiler_params=params(collective_id=0, has_side_effects=True),
        name="gather_right",
    )(right_factor)
    partial = pl.pallas_call(
        project,
        grid=(steps,),
        out_shape=jax.ShapeDtypeStruct((rows, rank), f32),
        in_specs=[cube, cube, fixed(cols, rank)], out_specs=stripe(rank),
        scratch_shapes=[pltpu.VMEM((cols, rank), bf16)] * 2,
        compiler_params=params(), name="project",
    )(momentum, gradient, right)
    chunk, total = rows // reps, reps * shard_n
    orthonormal = pl.pallas_call(
        functools.partial(orthonormalize, reps, shard_n),
        out_shape=jax.ShapeDtypeStruct((rows, rank), f32),
        in_specs=[vmem], out_specs=vmem,
        scratch_shapes=[
            pltpu.VMEM((rows, rank), f32),
            pltpu.VMEM((2, chunk, rank // 2), f32), pltpu.VMEM((2, chunk, rank // 2), f32),
            pltpu.VMEM((chunk, rank // 2), f32), pltpu.VMEM((chunk, rank // 2), f32),
            pltpu.VMEM((rank, rank), f32),
            pltpu.VMEM((total, rank // total, rank), f32),
            pltpu.VMEM((rank, rank), f32), pltpu.VMEM((rank, rank), f32),
            dma((12,)), dma((12,)), dma((total,)), dma((total,)), dma((total,)), dma((total,)),
        ],
        compiler_params=params(collective_id=1, has_side_effects=True),
        name="orthonormalize",
    )(partial)
    term = pl.pallas_call(
        factor_term,
        grid=(steps,),
        out_shape=jax.ShapeDtypeStruct((rank, cols), f32),
        in_specs=[cube, cube, stripe(rank)], out_specs=fixed(rank, cols),
        compiler_params=params(), name="factor_term",
    )(momentum, gradient, orthonormal)
    n1 = rank // 2 // reps
    factor = pl.pallas_call(
        functools.partial(sum_factor, reps, shard_n),
        out_shape=jax.ShapeDtypeStruct((rank, cols), f32),
        in_specs=[vmem], out_specs=vmem,
        scratch_shapes=[
            pltpu.VMEM((rank // 2, cols), f32),
            pltpu.VMEM((2, n1, cols // 2), f32), pltpu.VMEM((2, n1, cols // 2), f32),
            pltpu.VMEM((n1, cols // 2), f32), pltpu.VMEM((n1, cols // 2), f32),
            pltpu.VMEM((chips, n1 // chips, cols), f32), pltpu.VMEM((n1, cols), f32),
            dma((20,)), dma((20,)), dma((2 * chips,)), dma((2 * chips,)),
        ],
        compiler_params=params(collective_id=2, has_side_effects=True),
        name="sum_factor",
    )(term)
    new_momentum, update, new = pl.pallas_call(
        functools.partial(finish, math.sqrt(total_rows * cols / rank)),
        grid=(steps,),
        out_shape=(
            jax.ShapeDtypeStruct(momentum.shape, f32),
            jax.ShapeDtypeStruct((rows, cols), bf16),
            jax.ShapeDtypeStruct((rank, cols), f32),
        ),
        in_specs=[cube, cube, stripe(rank), fixed(rank, cols)],
        out_specs=(cube, stripe(cols), fixed(rank, cols)),
        scratch_shapes=[pltpu.VMEM((rank, cols), bf16), pltpu.VMEM((3 * rank, cols), bf16)],
        compiler_params=params(), name="finish",
    )(momentum, gradient, orthonormal, factor)
    own = cols // shard_n
    new_factor = lax.dynamic_slice_in_dim(new, lax.axis_index("fsdp") * own, own, axis=1).T
    return new_momentum, update, new_factor


def by_collectives(reps, shard_n, total_rows, momentum, gradient, right_factor):
    buffer = momentum[0] + gradient[0].astype(f32)
    partial = exact(buffer, lax.all_gather(right_factor, "fsdp", axis=0, tiled=True))
    projected = lax.psum(partial, "rep")
    gram_matrix = lax.psum(exact(projected, projected, TN), "fsdp")
    lower_factor = jnp.linalg.cholesky(gram_matrix)
    orthonormal = jax.scipy.linalg.solve_triangular(lower_factor, projected.T, lower=True).T
    scattered = lax.psum_scatter(
        exact(buffer, orthonormal, TN), "fsdp", scatter_dimension=0, tiled=True)
    own_factor = lax.psum(scattered, "rep") / reps
    full_factor = lax.all_gather(own_factor, "fsdp", axis=0, tiled=True)
    col_norms = jnp.sqrt(jnp.sum(full_factor * full_factor, axis=0) + epsilon)
    new_factor = own_factor / col_norms
    correction = exact(orthonormal, full_factor, NT)
    new_momentum = (buffer - (1.0 - decay_rate) * correction)[None]
    direction = exact(orthonormal, full_factor / col_norms, NT)
    scale = math.sqrt(total_rows * buffer.shape[1] / right_factor.shape[1])
    return new_momentum, (scale * direction).astype(bf16), new_factor


def solution(mesh):
    reps, shard_n = mesh.shape["rep"], mesh.shape["fsdp"]

    def shards(momentum, gradient, right_factor):
        rows, cols = momentum.shape[1:]
        rank = right_factor.shape[1]
        fits = (
            reps == 4 and shard_n % 2 == 0 and shard_n > 2 and rows % 128 == 0
            and (cols // shard_n) % 8 == 0 and cols % 256 == 0
            and rank % (8 * reps * shard_n) == 0
        )
        run = by_kernels if fits else by_collectives
        return run(reps, shard_n, rows * shard_n, momentum, gradient, right_factor)

    in_specs = (P("rep", "fsdp", None), P("rep", "fsdp", None), P("fsdp", None))
    out_specs = (P("rep", "fsdp", None), P("fsdp", None), P("fsdp", None))
    return jax.shard_map(shards, mesh=mesh, in_specs=in_specs, out_specs=out_specs, check_vma=False)
```
